32 devices in a mesh: lat: 4 (over z), lon: 8 (over y, x, core).
Axes of the slice: x: 2, y: 2, z: 4, core: 2. Of those that a mesh axis runs over, the one named last changes fastest.
Arguments:
- state: float32 [2, 3072, 6144], P(None, 'lat', 'lon'), may hold values from -6 to 6
- direction: float32 [2, 3072, 6144], P(None, 'lat', 'lon'), may hold values from -6 to 6
- diffusivity: bfloat16 [3072, 6144], P('lat', 'lon'), may hold values from 0.29882812 to 3
- inverses: bfloat16 [384, 8, 8, 12, 256], P(('lat', 'lon')), may hold values from -1.5 to 3
Outputs:
- preconditioned: float32 [2, 3072, 6144], P(None, 'lat', 'lon')
- jacobian_product: float32 [2, 3072, 6144], P(None, 'lat', 'lon')
The draws below stay inside these ranges and needn't reach their ends.
All inputs are finite; a program needn't handle non-finite values.
Results may differ from the reference program's by a relative error of at most 0.0003.
Values sent between devices are 32-bit elements; how exact they have to be, the bound alone decides.
No kernel may reach another device: no remote copies, remote signals or barrier semaphores. Data moves between devices by JAX's collectives and lax.ppermute only.
A program may use at most 128 MiB of HBM per device.

```python
import math
import jax
import jax.numpy as jnp
from jax import lax

CLAT = 768
NLAT = 3072
NLON = 6144
LEV = 2
ZSPLIT = 12
HALFZ = 256
BLK = 8


def draw_inverses(key, part):
    shape = (NLAT // BLK, BLK, BLK, ZSPLIT, HALFZ)
    diag_key, noise_key = jax.random.split(jax.random.fold_in(key, 11))
    lowest, highest = (0.2, 2.0)
    scales = jnp.exp(jax.random.uniform(diag_key, (NLAT // BLK, BLK, 1, ZSPLIT, HALFZ), jnp.float32, jnp.log(lowest), jnp.log(highest)))
    noise = jnp.clip(jax.random.normal(noise_key, shape, jnp.float32), -4.0, 4.0)
    identity = (jnp.arange(BLK)[:, None] == jnp.arange(BLK)[None, :]).astype(jnp.float32)[None, :, :, None, None]
    values = scales * (identity + 0.12 * noise * (1.0 - identity))
    return values.astype(jnp.bfloat16)


def levels(stream_key, shape, cuts, smallest, high):
    def one(dim, blocks):
        steps = jax.random.uniform(jax.random.fold_in(jax.random.fold_in(stream_key, 6), dim), (blocks,), jnp.float32, smallest / len(cuts), high / len(cuts))
        return jnp.repeat(jnp.exp(steps), shape[dim] // blocks).reshape((-1,) + (1,) * (len(shape) - dim - 1))

    loudness = one(*cuts[0])
    for cut in cuts[1:]:
        loudness = loudness * one(*cut)
    return loudness


def centred(stream_key, extent, deviation, most, cuts=(), kind=jnp.bfloat16):
    loudness = levels(stream_key, extent, cuts, -0.22, 0.18) if cuts else 1.0
    drawn = jax.random.normal(stream_key, extent, jnp.float32) * deviation * loudness
    return jnp.minimum(jnp.maximum(drawn, -most), most).astype(kind)


def setup_inputs(seed: int = 0) -> dict:
    key_of = jax.random.split(jax.random.key(seed), 5)
    state = centred(key_of[0], (LEV, NLAT, NLON), 1.0, 6.0, ((1, 4), (2, 8)), jnp.float32)
    direction = centred(key_of[1], (LEV, NLAT, NLON), 1.0, 6.0, ((1, 4), (2, 8)), jnp.float32)
    diffusivity = jnp.clip(jnp.exp(math.log(3.0) - 2.306499 * jax.random.uniform(key_of[2], (NLAT, NLON), jnp.float32) ** levels(key_of[2], (NLAT, NLON), ((0, 4), (1, 8)), -0.2, 0.2)), 0.29882812, 3.0).astype(jnp.bfloat16)
    inverses = draw_inverses(jax.random.fold_in(key_of[4], 71), 0)
    return dict(state=state, direction=direction, diffusivity=diffusivity, inverses=inverses)


zonal_tau = 0.1
merid_tau = 0.5
zonal_cap = 16.0
quad_coef = 0.25
step_size = 0.01


def lat_geometry(first_row, count, total):
    rows = (first_row + jnp.arange(count, dtype=jnp.int32)).astype(jnp.float32)
    limit = jnp.float32(total)
    cell_cos = jnp.sin(jnp.pi * (rows + 0.5) / limit)
    low_face = rows
    high_face = rows + 1.0
    face_low = jnp.where((low_face > 0.0) & (low_face < limit), jnp.sin(jnp.pi * low_face / limit), 0.0)
    face_high = jnp.where(high_face < limit, jnp.sin(jnp.pi * high_face / limit), 0.0)
    zonal_factor = jnp.minimum(1.0 / (cell_cos * cell_cos), zonal_cap)
    return cell_cos[:, None], face_low[:, None], face_high[:, None], zonal_factor[:, None]


def tendency(padded, kappa_field, cell_cos, face_low, face_high, zonal_factor):
    centre = padded[:, 1:-1, 1:-1]
    east_cell = padded[:, 1:-1, 2:]
    west_cell = padded[:, 1:-1, :-2]
    north_cell = padded[:, 2:, 1:-1]
    south_cell = padded[:, :-2, 1:-1]
    east_flux = zonal_tau * zonal_factor * (1.0 + quad_coef * jnp.square(0.5 * (centre + east_cell))) * (east_cell - centre)
    west_flux = zonal_tau * zonal_factor * (1.0 + quad_coef * jnp.square(0.5 * (centre + west_cell))) * (centre - west_cell)
    north_flux = merid_tau * face_high * (1.0 + quad_coef * jnp.square(0.5 * (centre + north_cell))) * (north_cell - centre)
    south_flux = merid_tau * face_low * (1.0 + quad_coef * jnp.square(0.5 * (centre + south_cell))) * (centre - south_cell)
    spread = (east_flux - west_flux) + (north_flux - south_flux) / cell_cos
    return centre - kappa_field * spread


def extend(field):
    field = jnp.concatenate([field[:, :, -1:], field, field[:, :, :1]], 2)
    return jnp.pad(field, ((0, 0), (1, 1), (0, 0)))


def reference(state, direction, diffusivity, inverses):
    bands = NLAT // CLAT
    band_ids = jnp.arange(bands, dtype=jnp.int32)

    def precondition(band):
        rows_in = lax.dynamic_slice_in_dim(direction, band * CLAT, CLAT, 1)
        blocks = lax.dynamic_slice_in_dim(inverses, band * (CLAT // BLK), CLAT // BLK, 0).astype(jnp.float32)
        spectrum = jnp.fft.rfft(rows_in, axis=-1)[..., : NLON // 2]
        spectrum = spectrum.reshape(LEV, CLAT // BLK, BLK, HALFZ, ZSPLIT)
        spectrum = jnp.swapaxes(spectrum, 3, 4)
        real_part = jnp.einsum("brskq,lbskq->lbrkq", blocks, spectrum.real.astype(jnp.float32))
        imag_part = jnp.einsum("brskq,lbskq->lbrkq", blocks, spectrum.imag.astype(jnp.float32))
        solved = lax.complex(real_part, imag_part)
        solved = jnp.swapaxes(solved, 3, 4).reshape(LEV, CLAT, NLON // 2)
        solved = jnp.concatenate([solved, jnp.zeros((LEV, CLAT, 1), solved.dtype)], 2)
        return jnp.fft.irfft(solved, n=NLON, axis=-1).astype(jnp.float32)

    pieces = lax.map(precondition, band_ids)
    preconditioned = jnp.transpose(pieces, (1, 0, 2, 3)).reshape(LEV, NLAT, NLON)
    state_pad = extend(state)
    field_pad = extend(preconditioned)

    def product(band):
        base_pad = lax.dynamic_slice_in_dim(state_pad, band * CLAT, CLAT + 2, 1)
        moved_pad = lax.dynamic_slice_in_dim(field_pad, band * CLAT, CLAT + 2, 1)
        kappa_field = lax.dynamic_slice_in_dim(diffusivity, band * CLAT, CLAT, 0).astype(jnp.float32)
        geometry = lat_geometry(band * CLAT, CLAT, NLAT)
        base = tendency(base_pad, kappa_field, *geometry)
        moved = tendency(base_pad + step_size * moved_pad, kappa_field, *geometry)
        return (moved - base) / step_size

    parts = lax.map(product, band_ids)
    jacobian_product = jnp.transpose(parts, (1, 0, 2, 3)).reshape(LEV, NLAT, NLON)
    return preconditioned, jacobian_product
```

```python
import functools
import math

import jax
import jax.numpy as jnp
from jax import lax
from jax.experimental import pallas as pl
from jax.experimental.pallas import tpu as pltpu
from jax.sharding import PartitionSpec as P


zonal_tau = 0.1
merid_tau = 0.5
zonal_cap = 16.0
step_size = 0.01


def scaled(value, factor):
    if value is None or abs(factor) < 1e-12:
        return None
    if abs(factor - 1.0) < 1e-12:
        return value
    if abs(factor + 1.0) < 1e-12:
        return -value
    return value * jnp.float32(factor)


def added(first, second, sign=1.0):
    if second is None:
        return first
    if first is None:
        return second if sign > 0 else -second
    return first + second if sign > 0 else first - second


def trig_sums(values, size, trig):
    sums = []
    for q in range(size // 4 + 1):
        parts = [None, None]
        groups = [{}, {}]
        for j, value in values:
            factor = trig(2.0 * math.pi * ((j * q) % size) / size)
            if abs(factor) < 1e-12:
                continue
            key = round(abs(factor), 9)
            total = groups[j % 2].get(key, (None, abs(factor)))[0]
            groups[j % 2][key] = (added(total, value, 1.0 if factor > 0 else -1.0), abs(factor))
        for parity in (0, 1):
            for total, factor in groups[parity].values():
                parts[parity] = added(parts[parity], scaled(total, factor))
        sums.append(parts)
    return sums


def real_outer(xs):
    size = len(xs)
    half = size // 2
    even = [(0, xs[0]), (half, xs[half])] + [(j, xs[j] + xs[size - j]) for j in range(1, half)]
    odd = [(j, xs[j] - xs[size - j]) for j in range(1, half)]
    re = [None] * (half + 1)
    im = [None] * (half + 1)
    for q, (a, b) in enumerate(trig_sums(even, size, math.cos)):
        re[q] = added(a, b)
        re[half - q] = added(a, b, -1.0)
    for q, (a, b) in enumerate(trig_sums(odd, size, math.sin)):
        total = added(a, b)
        im[q] = None if total is None else -total
        if q != half - q:
            im[half - q] = added(a, b, -1.0)
    return re, im


def real_outer_back(re, im, half):
    size = 2 * half
    xs = [None] * size
    cosines = trig_sums(list(enumerate(re)), size, math.cos)
    sines = trig_sums([(q, im[q]) for q in range(1, half)], size, math.sin)
    for j in range(size // 4 + 1):
        a, b = cosines[j]
        c, d = sines[j]
        even_part, odd_part = added(a, b), added(c, d)
        xs[j] = added(even_part, odd_part, -1.0)
        if j > 0:
            xs[size - j] = added(even_part, odd_part)
        even_part, odd_part = added(a, b, -1.0), added(d, c, -1.0)
        xs[half - j] = added(even_part, odd_part, -1.0)
        if j > 0:
            xs[half + j] = added(even_part, odd_part)
    return xs


def split_product(values, high, low):
    top = values.astype(jnp.bfloat16)
    rest = (values - top.astype(jnp.float32)).astype(jnp.bfloat16)
    dot = functools.partial(jnp.dot, preferred_element_type=jnp.float32)
    return dot(top, high) + (dot(rest, high) + dot(top, low))


def spectral_kernel(
    outer, inner, step_rows,
    y_ref, inv_ref, tc_ref, ts_ref, fh_ref, fl_ref, gh_ref, gl_ref,
    out_ref, z_ref, s_ref,
):
    half_inner = inner // 2
    half = outer // 2
    width = y_ref.shape[2]
    tile = math.gcd(math.gcd(inner, width), 256)
    groups = step_rows // 8
    step = pl.program_id(0)
    first = step * step_rows
    sources = y_ref.shape[0]
    share = out_ref.shape[1] - 8

    def place(j, h):
        n = j * inner + h * tile
        return n // width, n % width

    def forward(g, carry):
        rows = pl.ds(pl.multiple_of(g * 8, 8), 8)
        for h in range(inner // tile):
            cols = slice(h * tile, (h + 1) * tile)
            xs = []
            for j in range(outer):
                d, c = place(j, h)
                xs.append(y_ref[d, rows, c : c + tile])
            re, im = real_outer(xs)
            for q in range(outer):
                a, b = (re[q], im[q]) if q <= half else (re[outer - q], im[outer - q])
                if q > half and b is not None:
                    b = -b
                if q == 0:
                    zr, zi = a, jnp.zeros_like(a)
                else:
                    tc, ts = tc_ref[q, :, cols], ts_ref[q, :, cols]
                    if b is None:
                        zr, zi = a * tc, -(a * ts)
                    else:
                        zr, zi = a * tc + b * ts, b * tc - a * ts
                z_ref[q, rows, h * tile : (h + 1) * tile] = zr
                z_ref[q, rows, inner + h * tile : inner + (h + 1) * tile] = zi
        return carry

    lax.fori_loop(0, groups, forward, 0)
    flat = (outer * step_rows, 2 * inner)
    s_ref[...] = split_product(z_ref[...].reshape(flat), fh_ref[...], fl_ref[...]).reshape(s_ref.shape)

    lane = lax.broadcasted_iota(jnp.int32, (1, half_inner), 1)

    def solve(q, carry):
        weight = jnp.where((lane == 0) & (q == 0), 0.5, 1.0).astype(jnp.float32)
        for g in range(groups):
            re = im = None
            for s in range(8):
                factor = inv_ref[g, q, s].astype(jnp.float32)
                source = pl.ds(g * 8 + s, 8, stride=0)
                both = s_ref[q, source, :]
                sr, si = both[:, :half_inner], both[:, half_inner:]
                re = factor * sr if re is None else re + factor * sr
                im = factor * si if im is None else im + factor * si
            s_ref[q, g * 8 : g * 8 + 8, :half_inner] = re * weight
            s_ref[q, g * 8 : g * 8 + 8, half_inner:] = im * weight
        return carry

    lax.fori_loop(0, outer, solve, 0)
    flat = (outer * step_rows, 2 * half_inner)
    z_ref[...] = split_product(s_ref[...].reshape(flat), gh_ref[...], gl_ref[...]).reshape(z_ref.shape)

    def backward(g, carry):
        rows = pl.ds(pl.multiple_of(g * 8, 8), 8)
        target = pl.ds(pl.multiple_of(first + g * 8, 8), 8)
        for h in range(inner // tile):
            cols = slice(h * tile, (h + 1) * tile)

            def turned(q, want_im):
                ur = z_ref[q, rows, h * tile : (h + 1) * tile]
                if q == 0:
                    return ur, None
                ui = z_ref[q, rows, inner + h * tile : inner + (h + 1) * tile]
                tc, ts = tc_ref[q, :, cols], ts_ref[q, :, cols]
                return ur * tc - ui * ts, (ur * ts + ui * tc if want_im else None)

            re, im = [], []
            for q in range(half + 1):
                paired = 0 < q < half
                a, b = turned(q, paired)
                if paired:
                    c, d = turned(outer - q, True)
                    a, b = a + c, b - d
                re.append(a)
                im.append(b)
            for j, x in enumerate(real_outer_back(re, im, half)):
                d, c = place(j, h)
                out_ref[d, target, c : c + tile] = x
        return carry

    lax.fori_loop(0, groups, backward, 0)

    @pl.when(step == pl.num_programs(0) - 1)
    def _():
        for d in range(sources):
            here = slice(0, share)
            turned = jnp.transpose(out_ref[d, here, width - 128 :], (1, 0))
            out_ref[(d + 1) % sources, share : share + 1, here] = turned[127:128]
            turned = jnp.transpose(out_ref[d, here, :128], (1, 0))
            out_ref[(d - 1) % sources, share + 1 : share + 2, here] = turned[0:1]


def spectral(y, inverses, tables, step_rows):
    sources, row_count, width = y.shape
    outer = inverses.shape[1]
    inner = sources * width // outer
    half_inner = inverses.shape[4]
    block_rows = inverses.shape[2]
    whole = lambda array: pl.BlockSpec(array.shape, lambda i, n=array.ndim: (0,) * n)
    strip = pl.BlockSpec((sources, step_rows, width), lambda i: (0, i, 0))
    return pl.pallas_call(
        functools.partial(spectral_kernel, outer, inner, step_rows),
        grid=(row_count // step_rows,),
        in_specs=[
            strip,
            pl.BlockSpec(
                (step_rows // block_rows,) + inverses.shape[1:], lambda i: (i, 0, 0, 0, 0)
            ),
        ]
        + [whole(table) for table in tables],
        out_specs=pl.BlockSpec((sources, row_count + 8, width), lambda i: (0, 0, 0)),
        out_shape=jax.ShapeDtypeStruct((sources, row_count + 8, width), jnp.float32),
        scratch_shapes=[
            pltpu.VMEM((outer, step_rows, 2 * inner), jnp.float32),
            pltpu.VMEM((outer, step_rows, 2 * half_inner), jnp.float32),
        ],
        compiler_params=pltpu.CompilerParams(
            dimension_semantics=("arbitrary",), vmem_limit_bytes=36 * 1024 * 1024
        ),
        name="spectral",
    )(y, inverses, *tables)


def split_table(table):
    high = lax.reduce_precision(table, 8, 7)
    return high.astype(jnp.bfloat16), (table - high).astype(jnp.bfloat16)


def transform_tables(outer, inner):
    length = outer * inner
    half_inner = inner // 2
    outer_ids = jnp.arange(outer, dtype=jnp.int32)
    inner_ids = jnp.arange(inner, dtype=jnp.int32)
    half_ids = jnp.arange(half_inner, dtype=jnp.int32)
    twist = (
        2.0
        * jnp.pi
        * (outer_ids[:, None] * inner_ids[None, :] % length).astype(jnp.float32)
        / length
    )
    spread = lambda table: jnp.broadcast_to(table[:, None, :], (outer, 8, inner))
    angle = (
        2.0 * jnp.pi * (inner_ids[:, None] * half_ids[None, :] % inner).astype(jnp.float32) / inner
    )
    cos, sin = jnp.cos(angle), jnp.sin(angle)
    forward = jnp.concatenate(
        [jnp.concatenate([cos, -sin], 1), jnp.concatenate([sin, cos], 1)], 0
    )
    backward = jnp.concatenate(
        [jnp.concatenate([cos.T, sin.T], 1), jnp.concatenate([-sin.T, cos.T], 1)], 0
    ) * (2.0 / length)
    return (
        spread(jnp.cos(twist)),
        spread(jnp.sin(twist)),
        *split_table(forward),
        *split_table(backward),
    )


def stencil_kernel(
    share,
    state_ref, state_prev_ref, state_next_ref,
    pre_ref, pre_prev_ref, pre_next_ref, pre_first_ref, pre_last_ref,
    kappa_ref, column_ref, row_ref,
    *rest,
):
    pre_out_ref, jac_out_ref, side_ref = rest[-3:]
    i = pl.program_id(0)
    last = pl.num_programs(0) - 1
    width = state_ref.shape[2]
    strips = share // 8
    nudge = 0.25 * step_size

    def flux(low, high):
        total = low + high
        return (1.0 + total * total) * (high - low)

    lane = lax.broadcasted_iota(jnp.int32, (8, width), 1)
    sub = lax.broadcasted_iota(jnp.int32, (8, width), 0)

    table = jnp.transpose(column_ref[0], (1, 0))
    halo = jnp.transpose(pre_ref[0, share : share + 8, :128], (1, 0))
    side_ref[0, :, :8] = table
    side_ref[1, :, :8] = halo

    state_south = jnp.where(i == 0, row_ref[0:1, :], state_prev_ref[0, 7:8, :]) * 0.25
    state_north = jnp.where(i == last, row_ref[1:2, :], state_next_ref[0, 0:1, :]) * 0.25
    pre_south = jnp.where(i == 0, pre_last_ref[0, 3:4, :], pre_prev_ref[0, 7:8, :])
    pre_north = jnp.where(i == last, pre_first_ref[0, 2:3, :], pre_next_ref[0, 0:1, :])
    moved_south = state_south + pre_south * nudge
    moved_north = state_north + pre_north * nudge

    def load(g):
        rows = slice(g * 8, g * 8 + 8)
        state, pre = state_ref[0, rows, :] * 0.25, pre_ref[0, rows, :]
        return state, pre, state + pre * nudge

    here = load(0)
    below = flux(moved_south, here[2][:1]) - flux(state_south, here[0][:1])
    for g in range(strips):
        rows = slice(g * 8, g * 8 + 8)
        state, pre, moved = here
        if g + 1 < strips:
            here = load(g + 1)
            state_up, moved_up = here[0][:1], here[2][:1]
        else:
            state_up, moved_up = state_north, moved_north
        edge = lambda k: side_ref[0, rows, k : k + 1]
        zonal, north_factor, south_factor = edge(2), edge(3), edge(4)
        state_west, state_east = edge(0), edge(1)
        moved_west = state_west + side_ref[1, rows, 0:1] * nudge
        moved_east = state_east + side_ref[1, rows, 1:2] * nudge

        def from_east(field, column):
            return jnp.where(lane == width - 1, column, pltpu.roll(field, width - 1, 1))

        east = flux(moved, from_east(moved, moved_east)) - flux(state, from_east(state, state_east))
        west_edge = flux(moved_west, moved[:, :1]) - flux(state_west, state[:, :1])
        west = jnp.where(lane == 0, west_edge, pltpu.roll(east, 1, 1))
        spread = zonal * (east - west)

        def from_north(field, row):
            return pltpu.roll(jnp.where(sub == 0, row, field), 7, 0)

        north = flux(moved, from_north(moved, moved_up)) - flux(state, from_north(state, state_up))
        south = pltpu.roll(jnp.where(sub == 7, below, north), 1, 0)
        below = north[7:8]
        spread = spread + (north_factor * north - south_factor * south)
        pre_out_ref[0, rows, :] = pre
        jac_out_ref[0, rows, :] = pre - kappa_ref[rows, :].astype(jnp.float32) * spread


def stencil(level, state, pre, kappa, columns, rows, previous):
    _, row_count, width = state.shape
    steps = pre.shape[0]
    share = row_count // steps
    per = share // 8
    before = lambda i: jnp.maximum(i * per - 1, 0)
    after = lambda i: jnp.minimum((i + 1) * per, steps * per - 1)
    plane = pl.BlockSpec((1, share, width), lambda i: (level, i, 0))
    eight = lambda place: pl.BlockSpec((1, 8, width), place)
    in_specs = [
        plane,
        eight(lambda i: (level, before(i), 0)),
        eight(lambda i: (level, after(i), 0)),
        pl.BlockSpec((1, share + 8, width), lambda i: (i, 0, 0)),
        eight(lambda i: (jnp.maximum(i - 1, 0), per - 1, 0)),
        eight(lambda i: (jnp.minimum(i + 1, steps - 1), 0, 0)),
        eight(lambda i: (0, per, 0)),
        eight(lambda i: (steps - 1, per, 0)),
        pl.BlockSpec((share, width), lambda i: (i, 0)),
        pl.BlockSpec((1, 8, 128), lambda i: (i, 0, 0)),
        pl.BlockSpec((8, width), lambda i: (0, 0)),
    ]
    operands = [state, state, state, pre, pre, pre, pre, pre, kappa, columns, rows]
    aliases = {}
    if previous is not None:
        aliases = {len(operands): 0, len(operands) + 1: 1}
        operands += list(previous)
        in_specs += [pl.BlockSpec(memory_space=pl.ANY)] * 2
    shape = jax.ShapeDtypeStruct(state.shape, jnp.float32)
    return pl.pallas_call(
        functools.partial(stencil_kernel, share),
        grid=(steps,),
        in_specs=in_specs,
        out_specs=[plane, plane],
        out_shape=[shape, shape],
        scratch_shapes=[pltpu.VMEM((2, 128, 128), jnp.float32)],
        input_output_aliases=aliases,
        compiler_params=pltpu.CompilerParams(
            dimension_semantics=("arbitrary",), vmem_limit_bytes=12 * 1024 * 1024
        ),
        name="stencil",
    )(*operands)


def row_factors(first_row, count, total):
    rows = (first_row + jnp.arange(count, dtype=jnp.int32)).astype(jnp.float32)
    limit = jnp.float32(total)
    cell_cos = jnp.sin(jnp.pi * (rows + 0.5) / limit)
    high_face = rows + 1.0
    face_low = jnp.where((rows > 0.0) & (rows < limit), jnp.sin(jnp.pi * rows / limit), 0.0)
    face_high = jnp.where(high_face < limit, jnp.sin(jnp.pi * high_face / limit), 0.0)
    zonal_factor = jnp.minimum(1.0 / (cell_cos * cell_cos), zonal_cap)
    scale = 4.0 / step_size
    return (
        scale * zonal_tau * zonal_factor,
        scale * merid_tau * face_high / cell_cos,
        scale * merid_tau * face_low / cell_cos,
    )


def shifted(block, axis):
    count = lax.axis_size(axis)
    return lax.ppermute(block, axis, [(i, (i + 1) % count) for i in range(count)])


def shifted_back(block, axis):
    count = lax.axis_size(axis)
    return lax.ppermute(block, axis, [((i + 1) % count, i) for i in range(count)])


def exchange(block):
    return lax.all_to_all(block, "lon", 0, 0, tiled=True)


def on_device(state, direction, diffusivity, inverses):
    levels, local_rows, width = state.shape
    bands = lax.axis_size("lat")
    lons = lax.axis_size("lon")
    outer = inverses.shape[3]
    inner = 2 * inverses.shape[4]
    share = local_rows // lons
    step_rows = math.gcd(share, 48)

    pencils = []
    for level in range(levels):
        source = direction if level == 0 else lax.optimization_barrier(direction)
        pencils.append(source[level].reshape(lons, share, width))
    pencils = [exchange(pencil) for pencil in pencils]

    tables = transform_tables(outer, inner)
    arranged = jnp.transpose(inverses, (0, 3, 2, 1, 4))

    state_south = shifted(state[:, -1, :], "lat")
    state_north = shifted_back(state[:, 0, :], "lat")
    state_west = shifted(state[:, :, -1], "lon") * 0.25
    state_east = shifted_back(state[:, :, 0], "lon") * 0.25
    factors = row_factors(lax.axis_index("lat") * local_rows, local_rows, bands * local_rows)
    columns, rows = [], []
    for level in range(levels):
        lanes = jnp.stack([state_west[level], state_east[level], *factors], 0)
        lanes = jnp.transpose(lanes.reshape(-1, lons, share), (1, 0, 2))
        columns.append(jnp.pad(lanes, ((0, 0), (0, 8 - lanes.shape[1]), (0, 128 - share))))
        pair = jnp.stack([state_south[level], state_north[level]], 0)
        rows.append(jnp.pad(pair, ((0, 6), (0, 0))))

    fields = []
    for level in range(levels):
        block = spectral(pencils[level], arranged, tables, step_rows)
        north = shifted_back(block[:, 0, :], "lat")
        south = shifted(block[:, share - 1, :], "lat")
        block = block.at[:, share + 2 : share + 4, :].set(jnp.stack([north, south], 1))
        fields.append(exchange(block))

    outputs = None
    for level in range(levels):
        outputs = stencil(
            level, state, fields[level], diffusivity, columns[level], rows[level], outputs
        )
    return tuple(outputs)


def solution(mesh):
    return jax.shard_map(
        on_device,
        mesh=mesh,
        in_specs=(
            P(None, "lat", "lon"),
            P(None, "lat", "lon"),
            P("lat", "lon"),
            P(("lat", "lon"), None, None, None, None),
        ),
        out_specs=(P(None, "lat", "lon"), P(None, "lat", "lon")),
        check_vma=False,
    )
```
